32 devices in a mesh: dp: 4 (over x, y), sp: 8 (over z, core).
Axes of the slice: x: 2, y: 2, z: 4, core: 2. Of those that a mesh axis runs over, the one named last changes fastest.
Arguments:
- q: bfloat16 [128, 48, 128], P('dp'), parts along dimension 0
- k: bfloat16 [128, 8192, 8, 128], P('dp', 'sp'), parts along dimension 0
- v: bfloat16 [128, 8192, 8, 128], P('dp', 'sp'), parts along dimension 0
Outputs:
- q: bfloat16 [128, 48, 128], P('dp'), parts along dimension 0
There are 4 independent parts. The reference program is written for one: setup_inputs(seed, part) draws one part's arguments, and reference() takes and returns one part's arrays. A program takes and returns all parts, laid end to end along the dimension named above; each array names one.
All inputs are finite; a program needn't handle non-finite values.
Results may differ from the reference program's by a relative error of at most 0.012.
Values are sent between devices in bfloat16 or wider.
A program may use at most 2 GiB of HBM per device.

```python
import jax
import jax.numpy as jnp

BATCH = 32
CACHE = 8192
HEADS = 48
KV_HEADS = 8
HEAD = 128


def setup_inputs(seed: int = 0, part: int = 0) -> dict:
    kq, kk, kv = (jax.random.fold_in(k, part) for k in jax.random.split(jax.random.key(seed), 3))
    return {
        "q": (3 * jax.random.normal(kq, (BATCH, HEADS, HEAD), jnp.float32)).astype(jnp.bfloat16),
        "k": jax.random.normal(kk, (BATCH, CACHE, KV_HEADS, HEAD), jnp.float32).astype(jnp.bfloat16),
        "v": jax.random.normal(kv, (BATCH, CACHE, KV_HEADS, HEAD), jnp.float32).astype(jnp.bfloat16),
    }


def einsum(form, a, b):
    return jnp.einsum(form, a.astype(jnp.float32), b.astype(jnp.float32))


def reference(q, k, v):
    grouped = q.reshape(BATCH, KV_HEADS, -1, HEAD)
    scores = einsum("bgsd,bugd->bgsu", grouped, k) * HEAD**-0.5
    weights = jax.nn.softmax(scores, -1).astype(jnp.bfloat16)
    return einsum("bgsu,bugd->bgsd", weights, v).astype(jnp.bfloat16).reshape(BATCH, HEADS, HEAD)
```

```python
import functools
import math

import jax
import jax.numpy as jnp
from jax import lax
from jax.experimental import pallas as pl
from jax.experimental.pallas import tpu as pltpu
from jax.sharding import PartitionSpec as P

F32, BF16 = jnp.float32, jnp.bfloat16
RING = 6
LAG = 6
DIRECT = 2
TILE = 256


def kernel(group, q_ref, k_hbm, v_hbm, out_hbm, kbuf, vbuf, s0, s1, m0, m1, parts, stats, res, ksem, vsem, osem,
           po_send, ps_send, po_recv, ps_recv, r_send, r_recv):
    n, rows, d = k_hbm.shape
    heads = q_ref.shape[1]
    kv_heads = 8
    half = rows // 2
    tiles = half // TILE
    c = d**-0.5 * math.log2(math.e)
    me = lax.axis_index("sp")
    owned = n - DIRECT
    full = owned // group
    tail = full * group

    def kcopy(i):
        return pltpu.make_async_copy(k_hbm.at[i], kbuf.at[lax.rem(i, RING)], ksem.at[lax.rem(i, RING)])

    def vcopy(i):
        return pltpu.make_async_copy(v_hbm.at[i], vbuf.at[lax.rem(i, RING)], vsem.at[lax.rem(i, RING)])

    kcopy(0).start()
    for i in range(1, RING):
        kcopy(i).start()
        vcopy(i - 1).start()
    vcopy(RING - 1).start()

    barrier = pltpu.get_barrier_semaphore()
    for step in range(1, group):
        pl.semaphore_signal(barrier, inc=1, device_id={"sp": lax.rem(me + step, group)}, device_id_type=pl.DeviceIdType.MESH)

    shape = (heads, TILE)
    own_head = lax.broadcasted_iota(jnp.int32, shape, 0) // (heads // kv_heads) == lax.broadcasted_iota(jnp.int32, shape, 1) % kv_heads
    mask = jnp.concatenate([own_head, own_head], 0)
    row = lax.broadcasted_iota(jnp.int32, (heads, d), 0)
    lane = lax.broadcasted_iota(jnp.int32, (heads, d), 1)

    def side(ref, slot, t):
        return jnp.concatenate([ref[slot, t * TILE : (t + 1) * TILE, :], ref[slot, half + t * TILE : half + (t + 1) * TILE, :]], 1)

    def scores(i, s_ref, m_ref):
        slot = lax.rem(i, RING)
        q = q_ref[i]
        z = jnp.zeros_like(q)
        qq = jnp.concatenate([jnp.concatenate([q, z], 1), jnp.concatenate([z, q], 1)], 0)
        m = jnp.full((2 * heads, d), -jnp.inf, F32)
        for t in range(tiles):
            s = lax.dot_general(qq, side(kbuf, slot, t), (((1,), (1,)), ((), ())), preferred_element_type=F32)
            s = jnp.where(mask, s, -jnp.inf)
            s_ref[:, t * TILE : (t + 1) * TILE] = s
            m = jnp.maximum(m, jnp.maximum(s[:, :d], s[:, d:]))
        m_ref[...] = m

    def attend(i, s_ref, m_ref):
        slot = lax.rem(i, RING)
        m = m_ref[...]
        m = jnp.max(jnp.maximum(m[:heads], m[heads:]), 1, keepdims=True)
        m2 = jnp.concatenate([m, m], 0)
        l = jnp.zeros((2 * heads, d), F32)
        o = jnp.zeros((2 * heads, TILE), F32)
        for t in range(tiles):
            p = jnp.exp2((s_ref[:, t * TILE : (t + 1) * TILE] - m2) * c)
            l = l + (p[:, :d] + p[:, d:])
            o = o + lax.dot_general(p.astype(BF16), side(vbuf, slot, t), (((1,), (0,)), ((), ())), preferred_element_type=F32)
        l = jnp.sum(l[:heads] + l[heads:], 1, keepdims=True)
        parts[i, me] = (o[:heads, :d] + o[heads:, d:]).astype(BF16)
        stats[i, me] = jnp.sum(jnp.where(lane == row, m, jnp.where(lane == row + d // 2, l, 0.0)), 0, keepdims=True)

    def owner(i):
        return lax.rem(i + 2 * group - owned % group + 4, group)

    def index(i):
        if isinstance(i, int):
            return i // group if i < tail else full + i - tail
        return jnp.where(i < tail, i // group, full + i - tail)

    def part_copies(i, to):
        at = index(i)
        return [
            pltpu.make_async_remote_copy(ref.at[i, me], ref.at[i, me], send.at[at], recv.at[at], device_id={"sp": to}, device_id_type=pl.DeviceIdType.MESH)
            for ref, send, recv in ((parts, po_send, po_recv), (stats, ps_send, ps_recv))
        ]

    def result_copy(i, to):
        return pltpu.make_async_remote_copy(res.at[i], res.at[i], r_send.at[index(i)], r_recv.at[index(i)], device_id={"sp": to}, device_id_type=pl.DeviceIdType.MESH)

    def wait(ref, sem):
        pltpu.make_async_copy(ref, ref, sem).wait()

    def send_part(i):
        @pl.when(me != owner(i))
        def _():
            for copy in part_copies(i, owner(i)):
                copy.start()

    def send_all(copy_to):
        for step in range(1, group):
            copy_to(lax.rem(me + step, group))

    def wait_parts(i):
        wait(parts.at[i, : group - 1], po_recv.at[index(i)])
        wait(stats.at[i, : group - 1], ps_recv.at[index(i)])

    def together(i):
        st = stats[i, :, 0, :]
        w = jnp.exp2((st - jnp.max(st, 0, keepdims=True)) * c)
        w = w / jnp.sum(w * pltpu.roll(st, d // 2, 1), 0, keepdims=True)
        w = jnp.transpose(w)
        out = w[:heads, :1] * parts[i, 0].astype(F32)
        for s in range(1, group):
            out = out + w[:heads, s : s + 1] * parts[i, s].astype(F32)
        res[i] = out.astype(BF16)

    def owner_step(i):
        @pl.when(me == owner(i))
        def _():
            wait_parts(i)
            together(i)

    def owner_send(i):
        @pl.when(me == owner(i))
        def _():
            send_all(lambda to: result_copy(i, to).start())

    def exchange(i, back):
        if isinstance(i, int):
            if i >= back:
                return lambda f: f(i - back)
            return lambda f: None
        return lambda f: pl.when(i >= back)(lambda: f(i - back))

    def half_step(i, sa, ma, sb, mb):
        if not isinstance(i, int) or i + 1 < n:
            kcopy(i + 1).wait()
        vcopy(i).wait()
        if not isinstance(i, int) or i + 1 < n:
            scores(i + 1, sb, mb)
        attend(i, sa, ma)
        if not isinstance(i, int):
            @pl.when(i + 1 + RING < n)
            def _():
                kcopy(i + 1 + RING).start()

            @pl.when(i + RING < n)
            def _():
                vcopy(i + RING).start()
            send_part(i)
        else:
            for step in range(group - 1, 0, -1):
                for copy in part_copies(i, lax.rem(me + step, group)):
                    copy.start()
        exchange(i, LAG + 1)(owner_send)
        exchange(i, LAG)(owner_step)

    kcopy(0).wait()
    scores(0, s0, m0)
    kcopy(RING).start()
    pl.semaphore_wait(barrier, group - 1)

    def body(j, _):
        half_step(2 * j, s0, m0, s1, m1)
        half_step(2 * j + 1, s1, m1, s0, m0)
        return 0

    lax.fori_loop(0, owned // 2, body, 0)
    for i in range(owned, n):
        a, b = ((s0, m0), (s1, m1)) if i % 2 == 0 else ((s1, m1), (s0, m0))
        half_step(i, *a, *b)

    owner_send(n - 1 - LAG)
    for i in range(n - LAG, owned):
        owner_step(i)
        owner_send(i)
    for i in range(owned, n):
        wait_parts(i)
        together(i)

    for b in range(full):
        wait(res.at[: group - 1], r_recv.at[b])
    for i in range(tail, owned):
        @pl.when(me != owner(i))
        def _():
            wait(res.at[i], r_recv.at[index(i)])
    out = pltpu.make_async_copy(res, out_hbm, osem)
    out.start()

    for b in range(full):
        wait(parts.at[0, : group - 1], po_send.at[b])
        wait(stats.at[0, : group - 1], ps_send.at[b])
        wait(res.at[: group - 1], r_send.at[b])
    for i in range(tail, owned):
        @pl.when(me != owner(i))
        def _():
            wait(parts.at[i, 0], po_send.at[index(i)])
            wait(stats.at[i, 0], ps_send.at[index(i)])

        @pl.when(me == owner(i))
        def _():
            wait(res.at[: group - 1], r_send.at[index(i)])
    for i in range(owned, n):
        wait(parts.at[i, : group - 1], po_send.at[index(i)])
        wait(stats.at[i, : group - 1], ps_send.at[index(i)])
    out.wait()


def attention(group, q, k, v):
    n, heads, d = q.shape
    rows = k.shape[1] * k.shape[2]
    k, v = k.reshape(n, rows, d), v.reshape(n, rows, d)
    full = (n - DIRECT) // group
    sems = full + n - full * group
    anywhere = pl.BlockSpec(memory_space=pl.ANY)
    return pl.pallas_call(
        functools.partial(kernel, group),
        out_shape=jax.ShapeDtypeStruct((n, heads, d), BF16),
        in_specs=[pl.BlockSpec(memory_space=pltpu.VMEM), anywhere, anywhere],
        out_specs=anywhere,
        scratch_shapes=[
            pltpu.VMEM((RING, rows, d), BF16),
            pltpu.VMEM((RING, rows, d), BF16),
            pltpu.VMEM((2 * heads, rows // 2), F32),
            pltpu.VMEM((2 * heads, rows // 2), F32),
            pltpu.VMEM((2 * heads, d), F32),
            pltpu.VMEM((2 * heads, d), F32),
            pltpu.VMEM((n, group, heads, d), BF16),
            pltpu.VMEM((n, group, 1, d), F32),
            pltpu.VMEM((n, heads, d), BF16),
            pltpu.SemaphoreType.DMA((RING,)),
            pltpu.SemaphoreType.DMA((RING,)),
            pltpu.SemaphoreType.DMA,
        ]
        + [pltpu.SemaphoreType.DMA((sems,))] * 6,
        compiler_params=pltpu.CompilerParams(collective_id=0, has_side_effects=True, vmem_limit_bytes=48 * 2**20),
        cost_estimate=pl.CostEstimate(flops=8 * n * heads * rows * d, bytes_accessed=4 * n * rows * d, transcendentals=n * heads * rows),
    )(q, k, v)


def solution(mesh):
    cache = P("dp", "sp", None, None)
    return jax.shard_map(
        functools.partial(attention, mesh.shape["sp"]),
        mesh=mesh,
        in_specs=(P("dp", None, None), cache, cache),
        out_specs=P("dp", None, None),
        check_vma=False,
    )
```

```python
import functools
import math

import jax
import jax.numpy as jnp
from jax import lax
from jax.experimental import pallas as pl
from jax.experimental.pallas import tpu as pltpu
from jax.sharding import PartitionSpec as P

F32, BF16 = jnp.float32, jnp.bfloat16
RING = 6
LAG = 4
DIRECT = 1
UNROLL = 2
TILE = 256
PIECES = 4
MESH = pl.DeviceIdType.MESH


def kernel(group, q_hbm, k_hbm, v_hbm, res, qbuf, kbuf, vbuf, s0, s1, m0, m1, p0, p1, parts, stats, ksem, vsem, qsem, lsem,
           po_send, ps_send, po_recv, ps_recv, r_send, r_recv):
    n, rows, d = k_hbm.shape
    heads = qbuf.shape[1]
    kv_heads = 8
    half = rows // 2
    tiles = half // TILE
    c = d**-0.5 * math.log2(math.e)
    me = lax.axis_index("sp")
    owned = n - DIRECT
    full = owned // group
    tail = full * group
    last = n - 1
    piece = half // PIECES

    def kcopy(i):
        return pltpu.make_async_copy(k_hbm.at[i], kbuf.at[lax.rem(i, RING)], ksem.at[lax.rem(i, RING)])

    def qcopy(i):
        return pltpu.make_async_copy(q_hbm.at[i], qbuf.at[lax.rem(i, RING)], qsem.at[lax.rem(i, RING)])

    def vcopy(i):
        return pltpu.make_async_copy(v_hbm.at[i], vbuf.at[lax.rem(i, RING)], vsem.at[lax.rem(i, RING)])

    def last_copies(k):
        out = []
        for h in range(2):
            at = pl.ds(h * half + k * piece, piece)
            out.append(pltpu.make_async_copy(v_hbm.at[last, at], vbuf.at[last % RING, at], lsem.at[2 * k + h]))
        return out

    for i in range(RING):
        qcopy(i).start()
        kcopy(i).start()
        if i:
            vcopy(i - 1).start()
    vcopy(RING - 1).start()

    barrier = pltpu.get_barrier_semaphore()
    for step in range(1, group):
        pl.semaphore_signal(barrier, inc=1, device_id={"sp": lax.rem(me + step, group)}, device_id_type=MESH)

    shape = (heads, TILE)
    own_head = lax.broadcasted_iota(jnp.int32, shape, 0) // (heads // kv_heads) == lax.broadcasted_iota(jnp.int32, shape, 1) % kv_heads
    mask = jnp.concatenate([own_head, own_head], 0)
    row = lax.broadcasted_iota(jnp.int32, (heads, d), 0)
    lane = lax.broadcasted_iota(jnp.int32, (heads, d), 1)

    def side(ref, slot, t):
        return jnp.concatenate([ref[slot, t * TILE : (t + 1) * TILE, :], ref[slot, half + t * TILE : half + (t + 1) * TILE, :]], 1)

    def scores(i, s_ref, m_ref):
        slot = lax.rem(i, RING)
        q = qbuf[slot]
        z = jnp.zeros_like(q)
        qq = jnp.concatenate([jnp.concatenate([q, z], 1), jnp.concatenate([z, q], 1)], 0)
        m = jnp.full((2 * heads, d), -jnp.inf, F32)
        for t in range(tiles):
            s = lax.dot_general(qq, side(kbuf, slot, t), (((1,), (1,)), ((), ())), preferred_element_type=F32)
            s = jnp.where(mask, s, -jnp.inf)
            s_ref[:, t * TILE : (t + 1) * TILE] = s
            m = jnp.maximum(m, jnp.maximum(s[:, :d], s[:, d:]))
        m_ref[...] = m

    def weights(i, s_ref, m_ref):
        m = m_ref[...]
        m = jnp.max(jnp.maximum(m[:heads], m[heads:]), 1, keepdims=True)
        m2 = jnp.concatenate([m, m], 0)
        l = jnp.zeros((2 * heads, d), F32)
        for t in range(tiles):
            p = jnp.exp2((s_ref[:, t * TILE : (t + 1) * TILE] - m2) * c)
            l = l + (p[:, :d] + p[:, d:])
            yield t, p.astype(BF16)
        l = jnp.sum(l[:heads] + l[heads:], 1, keepdims=True)
        stats[i, me] = jnp.sum(jnp.where(lane == row, m, jnp.where(lane == row + d // 2, l, 0.0)), 0, keepdims=True)

    def values(i, o, t, p):
        return o + lax.dot_general(p, side(vbuf, lax.rem(i, RING), t), (((1,), (0,)), ((), ())), preferred_element_type=F32)

    def keep(i, o):
        parts[i, me] = (o[:heads, :d] + o[heads:, d:]).astype(BF16)

    def attend(i, s_ref, m_ref):
        o = jnp.zeros((2 * heads, TILE), F32)
        for t, p in weights(i, s_ref, m_ref):
            o = values(i, o, t, p)
        keep(i, o)

    def store_weights(i, s_ref, m_ref, p_ref):
        for t, p in weights(i, s_ref, m_ref):
            p_ref[:, t * TILE : (t + 1) * TILE] = p

    def owner(i):
        return lax.rem(4 * n + owned + 2 - i, group)

    def index(i):
        if isinstance(i, int):
            return i // group if i < tail else full + i - tail
        return jnp.where(i < tail, i // group, full + i - tail)

    def part_copies(i, to):
        at = index(i)
        return [
            pltpu.make_async_remote_copy(ref.at[i, me], ref.at[i, me], send.at[at], recv.at[at], device_id={"sp": to}, device_id_type=MESH)
            for ref, send, recv in ((parts, po_send, po_recv), (stats, ps_send, ps_recv))
        ]

    def result_copy(i, to):
        return pltpu.make_async_remote_copy(res.at[i], res.at[i], r_send.at[index(i)], r_recv.at[index(i)], device_id={"sp": to}, device_id_type=MESH)

    def wait(ref, sem):
        pltpu.make_async_copy(ref, ref, sem).wait()

    def send_part(i):
        @pl.when(me != owner(i))
        def _():
            for copy in part_copies(i, owner(i)):
                copy.start()

    def send_direct(i):
        for step in range(group - 1, 0, -1):
            for copy in part_copies(i, lax.rem(me + step, group)):
                copy.start()

    def wait_parts(i):
        wait(parts.at[i, : group - 1], po_recv.at[index(i)])
        wait(stats.at[i, : group - 1], ps_recv.at[index(i)])

    def together(i):
        st = stats[i, :, 0, :]
        w = jnp.exp2((st - jnp.max(st, 0, keepdims=True)) * c)
        w = w / jnp.sum(w * pltpu.roll(st, d // 2, 1), 0, keepdims=True)
        w = jnp.transpose(w)
        out = w[:heads, :1] * parts[i, 0].astype(F32)
        for s in range(1, group):
            out = out + w[:heads, s : s + 1] * parts[i, s].astype(F32)
        res[i] = out.astype(BF16)

    def owner_step(i):
        @pl.when(me == owner(i))
        def _():
            wait_parts(i)
            together(i)
            for step in range(1, group):
                result_copy(i, lax.rem(me + step, group)).start()

    buffers = ((s0, m0), (s1, m1))

    def stretch(i, count):
        for h in range(count):
            qcopy(i + 1 + h).wait()
            kcopy(i + 1 + h).wait()
            vcopy(i + h).wait()
        for h in range(count):
            scores(i + 1 + h, *buffers[(h + 1) % 2])
            attend(i + h, *buffers[h % 2])
        if not isinstance(i, int):
            for h in range(count):
                @pl.when(i + h + 1 + RING < n)
                def _():
                    qcopy(i + h + 1 + RING).start()
                    kcopy(i + h + 1 + RING).start()

                @pl.when(i + h + RING < last)
                def _():
                    vcopy(i + h + RING).start()

                @pl.when(i + h + RING == last)
                def _():
                    for k in range(PIECES):
                        for copy in last_copies(k):
                            copy.start()
        for h in range(count):
            send_part(i + h)
        for h in range(count):
            if isinstance(i, int):
                owner_step(i + h - LAG)
            else:
                pl.when(i + h >= LAG)(lambda: owner_step(i + h - LAG))

    qcopy(0).wait()
    kcopy(0).wait()
    scores(0, s0, m0)
    qcopy(RING).start()
    kcopy(RING).start()
    pl.semaphore_wait(barrier, group - 1)

    def body(j, _):
        stretch(UNROLL * j, UNROLL)
        return 0

    lax.fori_loop(0, (n - 4) // UNROLL, body, 0)
    stretch(n - 4, 2)

    qcopy(last).wait()
    kcopy(last).wait()
    scores(last, s1, m1)
    store_weights(last - 1, s0, m0, p0)
    owner_step(last - 1 - LAG)
    vcopy(last - 1).wait()
    store_weights(last, s1, m1, p1)
    o = jnp.zeros((2 * heads, TILE), F32)
    for t in range(tiles):
        o = values(last - 1, o, t, p0[:, t * TILE : (t + 1) * TILE])
    keep(last - 1, o)
    if last - 1 < owned:
        send_part(last - 1)
    else:
        send_direct(last - 1)
    o = jnp.zeros((2 * heads, TILE), F32)
    for t in range(tiles):
        if t % (tiles // PIECES) == 0:
            for copy in last_copies(t // (tiles // PIECES)):
                copy.wait()
        o = values(last, o, t, p1[:, t * TILE : (t + 1) * TILE])
    keep(last, o)
    send_direct(last)
    for i in range(last - LAG, owned):
        owner_step(i)
    for i in range(owned, n):
        wait_parts(i)
        together(i)

    for b in range(full):
        wait(parts.at[0, : group - 1], po_send.at[b])
        wait(stats.at[0, : group - 1], ps_send.at[b])
        wait(res.at[: group - 1], r_send.at[b])
        wait(res.at[: group - 1], r_recv.at[b])
    for i in range(tail, owned):
        @pl.when(me != owner(i))
        def _():
            wait(res.at[i], r_recv.at[index(i)])
            wait(parts.at[i, 0], po_send.at[index(i)])
            wait(stats.at[i, 0], ps_send.at[index(i)])

        @pl.when(me == owner(i))
        def _():
            wait(res.at[: group - 1], r_send.at[index(i)])
    for i in range(owned, n):
        wait(parts.at[i, : group - 1], po_send.at[index(i)])
        wait(stats.at[i, : group - 1], ps_send.at[index(i)])


def attention(group, q, k, v):
    n, heads, d = q.shape
    rows = k.shape[1] * k.shape[2]
    q = pltpu.with_memory_space_constraint(q, pltpu.HBM)
    k, v = k.reshape(n, rows, d), v.reshape(n, rows, d)
    full = (n - DIRECT) // group
    sems = full + n - full * group
    hbm = pl.BlockSpec(memory_space=pltpu.HBM)
    return pl.pallas_call(
        functools.partial(kernel, group),
        out_shape=jax.ShapeDtypeStruct((n, heads, d), BF16),
        in_specs=[hbm, hbm, hbm],
        out_specs=pl.BlockSpec(memory_space=pltpu.VMEM),
        scratch_shapes=[
            pltpu.VMEM((RING, heads, d), BF16),
            pltpu.VMEM((RING, rows, d), BF16),
            pltpu.VMEM((RING, rows, d), BF16),
            pltpu.VMEM((2 * heads, rows // 2), F32),
            pltpu.VMEM((2 * heads, rows // 2), F32),
            pltpu.VMEM((2 * heads, d), F32),
            pltpu.VMEM((2 * heads, d), F32),
            pltpu.VMEM((2 * heads, rows // 2), BF16),
            pltpu.VMEM((2 * heads, rows // 2), BF16),
            pltpu.VMEM((n, group, heads, d), BF16),
            pltpu.VMEM((n, group, 1, d), F32),
            pltpu.SemaphoreType.DMA((RING,)),
            pltpu.SemaphoreType.DMA((RING,)),
            pltpu.SemaphoreType.DMA((RING,)),
            pltpu.SemaphoreType.DMA((2 * PIECES,)),
        ]
        + [pltpu.SemaphoreType.DMA((sems,))] * 6,
        compiler_params=pltpu.CompilerParams(collective_id=0, has_side_effects=True, vmem_limit_bytes=46 * 2**20),
        cost_estimate=pl.CostEstimate(flops=8 * n * heads * rows * d, bytes_accessed=4 * n * rows * d, transcendentals=n * heads * rows),
    )(q, k, v)


def solution(mesh):
    cache = P("dp", "sp", None, None)
    return jax.shard_map(
        functools.partial(attention, mesh.shape["sp"]),
        mesh=mesh,
        in_specs=(P("dp", None, None), cache, cache),
        out_specs=P("dp", None, None),
        check_vma=False,
    )
```

```python
import functools
import math

import jax
import jax.numpy as jnp
from jax import lax
from jax.experimental import pallas as pl
from jax.experimental.pallas import tpu as pltpu
from jax.sharding import PartitionSpec as P

F32, BF16 = jnp.float32, jnp.bfloat16
RING = 6
LAG = 6
END_LAG = 4
DIRECT = 1
UNROLL = 2
TILE = 256
PIECES = 4
MESH = pl.DeviceIdType.MESH


def kernel(group, q_hbm, k_hbm, v_hbm, res, qbuf, kbuf, vbuf, s0, s1, m0, m1, p0, p1, parts, stats, ksem, vsem, qsem, lsem,
           po_send, ps_send, po_recv, ps_recv, r_send, r_recv):
    n, rows, d = k_hbm.shape
    heads = qbuf.shape[1]
    kv_heads = 8
    half = rows // 2
    tiles = half // TILE
    c = d**-0.5 * math.log2(math.e)
    me = lax.axis_index("sp")
    owned = n - DIRECT
    full = owned // group
    tail = full * group
    last = n - 1
    piece = half // PIECES

    def kcopy(i):
        return pltpu.make_async_copy(k_hbm.at[i], kbuf.at[lax.rem(i, RING)], ksem.at[lax.rem(i, RING)])

    def qcopy(i):
        return pltpu.make_async_copy(q_hbm.at[i], qbuf.at[lax.rem(i, RING)], qsem.at[lax.rem(i, RING)])

    def vcopy(i):
        return pltpu.make_async_copy(v_hbm.at[i], vbuf.at[lax.rem(i, RING)], vsem.at[lax.rem(i, RING)])

    def last_copies(k):
        out = []
        for h in range(2):
            at = pl.ds(h * half + k * piece, piece)
            out.append(pltpu.make_async_copy(v_hbm.at[last, at], vbuf.at[last % RING, at], lsem.at[2 * k + h]))
        return out

    for i in range(RING):
        qcopy(i).start()
        kcopy(i).start()
        if i:
            vcopy(i - 1).start()
    vcopy(RING - 1).start()

    barrier = pltpu.get_barrier_semaphore()
    for step in range(1, group):
        pl.semaphore_signal(barrier, inc=1, device_id={"sp": lax.rem(me + step, group)}, device_id_type=MESH)

    shape = (heads, TILE)
    own_head = lax.broadcasted_iota(jnp.int32, shape, 0) // (heads // kv_heads) == lax.broadcasted_iota(jnp.int32, shape, 1) % kv_heads
    mask = jnp.concatenate([own_head, own_head], 0)
    row = lax.broadcasted_iota(jnp.int32, (heads, d), 0)
    lane = lax.broadcasted_iota(jnp.int32, (heads, d), 1)

    def side(ref, slot, t):
        return jnp.concatenate([ref[slot, t * TILE : (t + 1) * TILE, :], ref[slot, half + t * TILE : half + (t + 1) * TILE, :]], 1)

    def scores(i, s_ref, m_ref):
        slot = lax.rem(i, RING)
        q = qbuf[slot]
        z = jnp.zeros_like(q)
        qq = jnp.concatenate([jnp.concatenate([q, z], 1), jnp.concatenate([z, q], 1)], 0)
        m = jnp.full((2 * heads, d), -jnp.inf, F32)
        for t in range(tiles):
            s = lax.dot_general(qq, side(kbuf, slot, t), (((1,), (1,)), ((), ())), preferred_element_type=F32)
            s = jnp.where(mask, s, -jnp.inf)
            s_ref[:, t * TILE : (t + 1) * TILE] = s
            m = jnp.maximum(m, jnp.maximum(s[:, :d], s[:, d:]))
        m_ref[...] = m

    def weights(i, s_ref, m_ref):
        m = m_ref[...]
        m = jnp.max(jnp.maximum(m[:heads], m[heads:]), 1, keepdims=True)
        m2 = jnp.concatenate([m, m], 0)
        l = jnp.zeros((2 * heads, d), F32)
        for t in range(tiles):
            p = jnp.exp2((s_ref[:, t * TILE : (t + 1) * TILE] - m2) * c)
            l = l + (p[:, :d] + p[:, d:])
            yield t, p.astype(BF16)
        l = jnp.sum(l[:heads] + l[heads:], 1, keepdims=True)
        stats[i, me] = jnp.sum(jnp.where(lane == row, m, jnp.where(lane == row + d // 2, l, 0.0)), 0, keepdims=True)

    def values(i, o, t, p):
        return o + lax.dot_general(p, side(vbuf, lax.rem(i, RING), t), (((1,), (0,)), ((), ())), preferred_element_type=F32)

    def keep(i, o):
        parts[i, me] = (o[:heads, :d] + o[heads:, d:]).astype(BF16)

    def attend(i, s_ref, m_ref):
        o = jnp.zeros((2 * heads, TILE), F32)
        for t, p in weights(i, s_ref, m_ref):
            o = values(i, o, t, p)
        keep(i, o)

    def store_weights(i, s_ref, m_ref, p_ref):
        for t, p in weights(i, s_ref, m_ref):
            p_ref[:, t * TILE : (t + 1) * TILE] = p

    def owner(i):
        return lax.rem(4 * n + owned + 2 - i, group)

    def index(i):
        if isinstance(i, int):
            return i // group if i < tail else full + i - tail
        return jnp.where(i < tail, i // group, full + i - tail)

    def part_copies(i, to):
        at = index(i)
        return [
            pltpu.make_async_remote_copy(ref.at[i, me], ref.at[i, me], send.at[at], recv.at[at], device_id={"sp": to}, device_id_type=MESH)
            for ref, send, recv in ((parts, po_send, po_recv), (stats, ps_send, ps_recv))
        ]

    def result_copy(i, to):
        return pltpu.make_async_remote_copy(res.at[i], res.at[i], r_send.at[index(i)], r_recv.at[index(i)], device_id={"sp": to}, device_id_type=MESH)

    def wait(ref, sem):
        pltpu.make_async_copy(ref, ref, sem).wait()

    def send_part(i):
        @pl.when(me != owner(i))
        def _():
            for copy in part_copies(i, owner(i)):
                copy.start()

    def send_direct(i):
        for step in range(group - 1, 0, -1):
            for copy in part_copies(i, lax.rem(me + step, group)):
                copy.start()

    def wait_parts(i):
        wait(parts.at[i, : group - 1], po_recv.at[index(i)])
        wait(stats.at[i, : group - 1], ps_recv.at[index(i)])

    def together(i):
        st = stats[i, :, 0, :]
        w = jnp.exp2((st - jnp.max(st, 0, keepdims=True)) * c)
        w = w / jnp.sum(w * pltpu.roll(st, d // 2, 1), 0, keepdims=True)
        w = jnp.transpose(w)
        out = w[:heads, :1] * parts[i, 0].astype(F32)
        for s in range(1, group):
            out = out + w[:heads, s : s + 1] * parts[i, s].astype(F32)
        res[i] = out.astype(BF16)

    def owner_step(i):
        @pl.when(me == owner(i))
        def _():
            wait_parts(i)
            together(i)
            for step in range(1, group):
                result_copy(i, lax.rem(me + step, group)).start()

    buffers = ((s0, m0), (s1, m1))

    def stretch(i, count):
        for h in range(count):
            qcopy(i + 1 + h).wait()
            kcopy(i + 1 + h).wait()
            vcopy(i + h).wait()
        for h in range(count):
            scores(i + 1 + h, *buffers[(h + 1) % 2])
            attend(i + h, *buffers[h % 2])
        if not isinstance(i, int):
            for h in range(count):
                @pl.when(i + h + 1 + RING < n)
                def _():
                    qcopy(i + h + 1 + RING).start()
                    kcopy(i + h + 1 + RING).start()

                @pl.when(i + h + RING < last)
                def _():
                    vcopy(i + h + RING).start()

                @pl.when(i + h + RING == last)
                def _():
                    for k in range(PIECES):
                        for copy in last_copies(k):
                            copy.start()
        for h in range(count):
            send_part(i + h)
        if isinstance(i, int):
            for x in range(i - LAG, i + count - END_LAG):
                owner_step(x)
            return
        for h in range(count):
            pl.when(i + h >= LAG)(lambda: owner_step(i + h - LAG))

    qcopy(0).wait()
    kcopy(0).wait()
    scores(0, s0, m0)
    qcopy(RING).start()
    kcopy(RING).start()
    pl.semaphore_wait(barrier, group - 1)

    def body(j, _):
        stretch(UNROLL * j, UNROLL)
        return 0

    lax.fori_loop(0, (n - 4) // UNROLL, body, 0)
    stretch(n - 4, 2)

    qcopy(last).wait()
    kcopy(last).wait()
    scores(last, s1, m1)
    store_weights(last - 1, s0, m0, p0)
    owner_step(last - 1 - END_LAG)
    vcopy(last - 1).wait()
    store_weights(last, s1, m1, p1)
    o = jnp.zeros((2 * heads, TILE), F32)
    for t in range(tiles):
        o = values(last - 1, o, t, p0[:, t * TILE : (t + 1) * TILE])
    keep(last - 1, o)
    if last - 1 < owned:
        send_part(last - 1)
    else:
        send_direct(last - 1)
    o = jnp.zeros((2 * heads, TILE), F32)
    for t in range(tiles):
        if t % (tiles // PIECES) == 0:
            for copy in last_copies(t // (tiles // PIECES)):
                copy.wait()
        o = values(last, o, t, p1[:, t * TILE : (t + 1) * TILE])
    keep(last, o)
    send_direct(last)
    for i in range(last - END_LAG, owned):
        owner_step(i)
    for i in range(owned, n):
        wait_parts(i)
        together(i)

    for b in range(full):
        wait(parts.at[0, : group - 1], po_send.at[b])
        wait(stats.at[0, : group - 1], ps_send.at[b])
        wait(res.at[: group - 1], r_send.at[b])
        wait(res.at[: group - 1], r_recv.at[b])
    for i in range(tail, owned):
        @pl.when(me != owner(i))
        def _():
            wait(res.at[i], r_recv.at[index(i)])
            wait(parts.at[i, 0], po_send.at[index(i)])
            wait(stats.at[i, 0], ps_send.at[index(i)])

        @pl.when(me == owner(i))
        def _():
            wait(res.at[: group - 1], r_send.at[index(i)])
    for i in range(owned, n):
        wait(parts.at[i, : group - 1], po_send.at[index(i)])
        wait(stats.at[i, : group - 1], ps_send.at[index(i)])


def attention(group, q, k, v):
    n, heads, d = q.shape
    rows = k.shape[1] * k.shape[2]
    q = pltpu.with_memory_space_constraint(q, pltpu.HBM)
    k, v = k.reshape(n, rows, d), v.reshape(n, rows, d)
    full = (n - DIRECT) // group
    sems = full + n - full * group
    hbm = pl.BlockSpec(memory_space=pltpu.HBM)
    return pl.pallas_call(
        functools.partial(kernel, group),
        out_shape=jax.ShapeDtypeStruct((n, heads, d), BF16),
        in_specs=[hbm, hbm, hbm],
        out_specs=pl.BlockSpec(memory_space=pltpu.VMEM),
        scratch_shapes=[
            pltpu.VMEM((RING, heads, d), BF16),
            pltpu.VMEM((RING, rows, d), BF16),
            pltpu.VMEM((RING, rows, d), BF16),
            pltpu.VMEM((2 * heads, rows // 2), F32),
            pltpu.VMEM((2 * heads, rows // 2), F32),
            pltpu.VMEM((2 * heads, d), F32),
            pltpu.VMEM((2 * heads, d), F32),
            pltpu.VMEM((2 * heads, rows // 2), BF16),
            pltpu.VMEM((2 * heads, rows // 2), BF16),
            pltpu.VMEM((n, group, heads, d), BF16),
            pltpu.VMEM((n, group, 1, d), F32),
            pltpu.SemaphoreType.DMA((RING,)),
            pltpu.SemaphoreType.DMA((RING,)),
            pltpu.SemaphoreType.DMA((RING,)),
            pltpu.SemaphoreType.DMA((2 * PIECES,)),
        ]
        + [pltpu.SemaphoreType.DMA((sems,))] * 6,
        compiler_params=pltpu.CompilerParams(collective_id=0, has_side_effects=True, vmem_limit_bytes=46 * 2**20),
        cost_estimate=pl.CostEstimate(flops=8 * n * heads * rows * d, bytes_accessed=4 * n * rows * d, transcendentals=n * heads * rows),
    )(q, k, v)


def solution(mesh):
    cache = P("dp", "sp", None, None)
    return jax.shard_map(
        functools.partial(attention, mesh.shape["sp"]),
        mesh=mesh,
        in_specs=(P("dp", None, None), cache, cache),
        out_specs=P("dp", None, None),
        check_vma=False,
    )
```
